32 devices in a mesh: seq: 16 (over z, y, core), head: 2 (over x).
Axes of the slice: x: 2, y: 2, z: 4, core: 2. Of those that a mesh axis runs over, the one named last changes fastest.
Arguments:
- tokens: bfloat16 [8192, 1024], P('seq'), may hold values from -24 to 24
- norm_attn: float32 [1024], replicated, may hold values from 0.5 to 1.5
- self_qkv: bfloat16 [3, 1024, 1024], P(None, None, 'head'), may hold values from -4 to 4
- self_out: bfloat16 [1024, 1024], P('head'), may hold values from -0.1875 to 0.1875
- norm_ffn: float32 [1024], replicated, may hold values from 0.5 to 1.5
- ffn_in: bfloat16 [2, 1024, 2816], P(None, None, 'head'), may hold values from -0.1875 to 0.1875
- ffn_out: bfloat16 [2816, 1024], P('head'), may hold values from -0.109375 to 0.109375
- norm_final: float32 [1024], replicated, may hold values from 0.5 to 1.5
- pad_lengths: int32 [16], replicated, may hold values from 64 to 512
- targets: bfloat16 [512, 1024], replicated, may hold values from -8 to 8
- target_lengths: int32 [4], replicated, may hold values from 32 to 128
- norm_cross: float32 [1024], replicated, may hold values from 0.1 to 1.9
- cross_query: bfloat16 [1024, 1024], P(None, 'head'), may hold values from -4 to 4
- cross_kv: bfloat16 [2, 1024, 1024], P(None, None, 'head'), may hold values from -4 to 4
- cross_out: bfloat16 [1024, 1024], P('head'), may hold values from -4 to 4
Outputs:
- encoded: bfloat16 [8192, 1024], P('seq')
- decoded: bfloat16 [512, 1024], replicated
The draws below stay inside these ranges and needn't reach their ends.
All inputs are finite; a program needn't handle non-finite values.
Results may differ from the reference program's by a relative error of at most 0.033.
Values may be sent and summed in bfloat16 or wider, within the bound.
No kernel may reach another device: no remote copies, remote signals or barrier semaphores. Data moves between devices by JAX's collectives and lax.ppermute only.
A program may use at most 128 MiB of HBM per device.

```python
import math
import jax
import jax.numpy as jnp
from jax import lax

D = 1024
HEADS = 16
HD = 64
FF = 2816
TOK_DEV = 512
TGT_SEQS = 4
TGT_LEN = 128
TOKENS = 8192
TGT = 512
BLOCKS = 16


def plant_strength():
    return math.sqrt(300.0 * math.sqrt(HD) / D)


def plant_vectors(seed_key):
    base_key = jax.random.fold_in(seed_key, 9001)
    direction = jax.random.normal(jax.random.fold_in(base_key, 1), (D,), jnp.float32)
    direction = direction / jnp.sqrt(jnp.sum(direction * direction))
    target_dir = jax.random.normal(jax.random.fold_in(base_key, 2), (HEADS, HD), jnp.float32)
    target_dir = target_dir / jnp.sqrt(jnp.sum(target_dir * target_dir, axis=1, keepdims=True))
    return (direction, target_dir.reshape(HEADS * HD))


def projection(seed_key, salt, planted):
    matrix = jax.random.normal(jax.random.fold_in(seed_key, salt), (planted.shape[0], D, HEADS * HD), jnp.float32) * D ** (-0.5)
    matrix = jnp.clip(matrix, -3.5, 3.5)
    direction, target_dir = plant_vectors(seed_key)
    bump = plant_strength() * jnp.outer(direction, target_dir)
    matrix = matrix + planted[:, None, None] * bump[None, :, :]
    return matrix


def draw_self_qkv(seed_key, part_index):
    return projection(seed_key, 11, jnp.array([1.0, 1.0, 0.0], jnp.float32)).astype(jnp.bfloat16)


def draw_cross_query(seed_key, part_index):
    return projection(seed_key, 12, jnp.array([1.0], jnp.float32))[0].astype(jnp.bfloat16)


def draw_cross_kv(seed_key, part_index):
    return projection(seed_key, 13, jnp.array([1.0, 0.0], jnp.float32)).astype(jnp.bfloat16)


def draw_tokens(seed_key, part_index):
    rows_drawn = jnp.clip(jax.random.normal(jax.random.fold_in(seed_key, 21), (TOKENS, D), jnp.float32), -6.0, 6.0)
    direction, target_dir = plant_vectors(seed_key)
    row_ids = jnp.arange(TOKENS, dtype=jnp.int32)[:, None]
    picked = (jax.random.randint(jax.random.fold_in(seed_key, 22), (TOKENS, 1), 0, 32) == 0) | (row_ids % (4 * TOK_DEV) == 0)
    planted_rows = 128.0 * direction[None, :] + 96.0 / math.sqrt(D) * rows_drawn
    rows_drawn = jnp.where(picked, planted_rows, rows_drawn)
    return jnp.clip(rows_drawn, -24.0, 24.0).astype(jnp.bfloat16)


def draw_targets(seed_key, part_index):
    rows_drawn = jnp.clip(jax.random.normal(jax.random.fold_in(seed_key, 31), (TGT, D), jnp.float32), -6.0, 6.0)
    direction, target_dir = plant_vectors(seed_key)
    row_ids = jnp.arange(TGT, dtype=jnp.int32)[:, None]
    picked = (jax.random.randint(jax.random.fold_in(seed_key, 32), (TGT, 1), 0, 16) == 0) | (row_ids == 0)
    rows_drawn = jnp.where(picked, 32.0 * direction[None, :], rows_drawn)
    return jnp.clip(rows_drawn, -8.0, 8.0).astype(jnp.bfloat16)


def set_ends(drawn, own_key, smallest, top_value):
    longest = drawn.shape.index(max(drawn.shape))
    spots = []
    for shift in (0, 1):
        where = [jax.random.randint(jax.random.fold_in(own_key, axis), (), 0, length) for axis, length in enumerate(drawn.shape)]
        where[longest] = (where[longest] + shift) % drawn.shape[longest]
        spots.append(tuple(where))
    return drawn.at[spots[0]].set(smallest).at[spots[1]].set(top_value)


def levels(own_key, shape, shards, least, largest):
    def one(axis_at, shards_of):
        steps = jax.random.uniform(jax.random.fold_in(jax.random.fold_in(own_key, 6), axis_at), (shards_of,), jnp.float32, least / len(shards), largest / len(shards))
        return jnp.repeat(jnp.exp(steps), shape[axis_at] // shards_of).reshape((-1,) + (1,) * (len(shape) - axis_at - 1))

    factor_of = one(*shards[0])
    for cut in shards[1:]:
        factor_of = factor_of * one(*cut)
    return factor_of


def scatter_about(stream_key, extent, scale, reach, cuts=(), held_as=jnp.bfloat16):
    loudness = levels(stream_key, extent, cuts, -0.22, 0.18) if cuts else 1.0
    values = jax.random.normal(stream_key, extent, jnp.float32) * scale * loudness
    return jnp.minimum(jnp.maximum(values, -reach), reach).astype(held_as)


def setup_inputs(seed: int = 0) -> dict:
    key_of = jax.random.split(jax.random.key(seed), 16)
    tokens = draw_tokens(jax.random.fold_in(key_of[15], 71), 0)
    norm_attn = jnp.clip(1.0 + 0.1 * jax.random.normal(key_of[1], (D,), jnp.float32), 0.5, 1.5)
    self_qkv = draw_self_qkv(jax.random.fold_in(key_of[15], 71), 0)
    self_out = scatter_about(key_of[3], (HEADS * HD, D), (HEADS * HD) ** -0.5, 0.1875, ((0, 2),))
    norm_ffn = jnp.clip(1.0 + 0.1 * jax.random.normal(key_of[4], (D,), jnp.float32), 0.5, 1.5)
    ffn_in = scatter_about(key_of[5], (2, D, FF), D ** -0.5, 0.1875, ((2, 2),))
    ffn_out = scatter_about(key_of[6], (FF, D), FF ** -0.5, 0.109375, ((0, 2),))
    norm_final = jnp.clip(1.0 + 0.1 * jax.random.normal(key_of[7], (D,), jnp.float32), 0.5, 1.5)
    pad_lengths = set_ends(jax.random.randint(key_of[8], (BLOCKS,), TOK_DEV // 8, TOK_DEV + 1), jax.random.fold_in(key_of[8], 1), TOK_DEV // 8, TOK_DEV).astype(jnp.int32)
    targets = draw_targets(jax.random.fold_in(key_of[15], 71), 0)
    target_lengths = set_ends(jax.random.randint(key_of[10], (TGT_SEQS,), TGT_LEN // 4, TGT_LEN + 1), jax.random.fold_in(key_of[10], 1), TGT_LEN // 4, TGT_LEN).astype(jnp.int32)
    norm_cross = jnp.clip(1.0 + 0.18 * jax.random.normal(key_of[11], (D,), jnp.float32), 0.1, 1.9)
    cross_query = draw_cross_query(jax.random.fold_in(key_of[15], 71), 0)
    cross_kv = draw_cross_kv(jax.random.fold_in(key_of[15], 71), 0)
    cross_out = scatter_about(key_of[14], (HEADS * HD, D), (8.0 / (HEADS * HD) ** 0.5), 4.0, ((0, 2),))
    return {"tokens": tokens, "norm_attn": norm_attn, "self_qkv": self_qkv, "self_out": self_out, "norm_ffn": norm_ffn, "ffn_in": ffn_in, "ffn_out": ffn_out, "norm_final": norm_final, "pad_lengths": pad_lengths, "targets": targets, "target_lengths": target_lengths, "norm_cross": norm_cross, "cross_query": cross_query, "cross_kv": cross_kv, "cross_out": cross_out}


epsilon = 1e-06
masked_score = -1e+30

def rms_norm(values, gain_vector):
    widened = values.astype(jnp.float32)
    return widened * lax.rsqrt(lax.optimization_barrier(jnp.mean(widened * widened, axis=-1, keepdims=True)) + epsilon) * gain_vector.astype(jnp.float32)

def attend(queries, keys, values, live_keys):
    query_count = queries.shape[0]
    key_count = keys.shape[0]
    query_heads = queries.reshape(query_count, HEADS, HD).transpose(1, 0, 2)
    key_heads = keys.reshape(key_count, HEADS, HD).transpose(1, 0, 2)
    value_heads = values.reshape(key_count, HEADS, HD).transpose(1, 0, 2)
    block_rows = math.gcd(query_count, 1024)
    scaling = HD ** (-0.5)

    def one_head(head_parts):
        head_queries, head_keys, head_values = head_parts
        blocked = head_queries.reshape(query_count // block_rows, block_rows, HD)

        def one_block(block_queries):
            scores = jnp.dot(block_queries, head_keys.T, preferred_element_type=jnp.float32) * scaling
            scores = jnp.where(live_keys[None, :], scores, masked_score)
            row_max = lax.optimization_barrier(jnp.max(scores, axis=1, keepdims=True))
            weights = jnp.where(live_keys[None, :], jnp.exp(scores - row_max), 0.0)
            weight_sum = lax.optimization_barrier(jnp.sum(weights, axis=1, keepdims=True))
            mixed_rows = jnp.dot(weights.astype(jnp.bfloat16), head_values, preferred_element_type=jnp.float32)
            return mixed_rows / weight_sum
        return lax.map(one_block, blocked).reshape(query_count, HD)
    per_head = lax.map(one_head, (query_heads, key_heads, value_heads))
    return per_head.transpose(1, 0, 2).reshape(query_count, HEADS * HD).astype(jnp.bfloat16)

def reference(tokens, norm_attn, self_qkv, self_out, norm_ffn, ffn_in, ffn_out, norm_final, pad_lengths, targets, target_lengths, norm_cross, cross_query, cross_kv, cross_out):
    normed = rms_norm(tokens, norm_attn).astype(jnp.bfloat16)
    queries = jnp.dot(normed, self_qkv[0], preferred_element_type=jnp.float32).astype(jnp.bfloat16)
    keys = jnp.dot(normed, self_qkv[1], preferred_element_type=jnp.float32).astype(jnp.bfloat16)
    values = jnp.dot(normed, self_qkv[2], preferred_element_type=jnp.float32).astype(jnp.bfloat16)
    positions = jnp.arange(TOKENS, dtype=jnp.int32)
    live = positions % TOK_DEV < jnp.repeat(pad_lengths, TOK_DEV, total_repeat_length=TOKENS)
    context = attend(queries, keys, values, live)
    hidden_in = tokens.astype(jnp.float32) + jnp.dot(context, self_out, preferred_element_type=jnp.float32)
    ffn_normed = rms_norm(hidden_in, norm_ffn).astype(jnp.bfloat16)
    gate_proj = jnp.dot(ffn_normed, ffn_in[0], preferred_element_type=jnp.float32)
    up_proj = jnp.dot(ffn_normed, ffn_in[1], preferred_element_type=jnp.float32)
    activated = (jax.nn.gelu(gate_proj, approximate=True) * up_proj).astype(jnp.bfloat16)
    final_in = hidden_in + jnp.dot(activated, ffn_out, preferred_element_type=jnp.float32)
    encoded = rms_norm(final_in, norm_final).astype(jnp.bfloat16)
    cross_normed = rms_norm(targets, norm_cross).astype(jnp.bfloat16)
    cross_queries = jnp.dot(cross_normed, cross_query, preferred_element_type=jnp.float32).astype(jnp.bfloat16)
    cross_keys = jnp.dot(encoded, cross_kv[0], preferred_element_type=jnp.float32).astype(jnp.bfloat16)
    cross_values = jnp.dot(encoded, cross_kv[1], preferred_element_type=jnp.float32).astype(jnp.bfloat16)
    cross_context = attend(cross_queries, cross_keys, cross_values, live)
    slots = jnp.arange(TGT, dtype=jnp.int32)
    target_live = slots % TGT_LEN < jnp.repeat(target_lengths, TGT_LEN, total_repeat_length=TGT)
    cross_total = jnp.dot(cross_context, cross_out, preferred_element_type=jnp.float32)
    decoded = (targets.astype(jnp.float32) + jnp.where(target_live[:, None], cross_total, 0.0)).astype(jnp.bfloat16)
    return (encoded, decoded)
```

```python
import functools
import math

import jax
import jax.numpy as jnp
from jax import lax
from jax.experimental import pallas as pl
from jax.experimental.pallas import tpu as pltpu
from jax.sharding import PartitionSpec as P

HD = 64
TOK_DEV = 512
TGT_LEN = 128
PAIR = 2 * HD
PIECE = 128

epsilon = 1e-06
masked_score = -1e30
LOG2E = math.log2(math.e)


def rms_norm(values, gain_vector):
    widened = values.astype(jnp.float32)
    return (
        widened
        * lax.rsqrt(jnp.mean(widened * widened, axis=-1, keepdims=True) + epsilon)
        * gain_vector
    )


def dot32(a, b):
    return jnp.dot(a, b, preferred_element_type=jnp.float32)


def flash_kernel(lens, q_ref, k_ref, v_ref, *refs, blocks, finish):
    if finish:
        out_ref, m_s, acc_s = refs
    else:
        out_ref, stat_ref, m_s, acc_s = refs
    j = pl.program_id(1)
    factor = HD ** (-0.5) * LOG2E

    @pl.when(j == 0)
    def _():
        m_s[...] = jnp.full(m_s.shape, masked_score, jnp.float32)
        acc_s[...] = jnp.zeros(acc_s.shape, jnp.float32)

    live = lens[j]
    pieces = (live + PIECE - 1) // PIECE

    def run(count):
        width = count * PIECE
        v_t = v_ref[:width, :].T
        ones = jnp.ones((16, width), jnp.bfloat16)
        alive = lax.broadcasted_iota(jnp.int32, (PIECE, 1), 0) < live - (width - PIECE)
        scores = []
        for h in range(2):
            cols = slice(h * HD, (h + 1) * HD)
            s = lax.dot_general(
                k_ref[:width, cols],
                q_ref[:, cols],
                (((1,), (1,)), ((), ())),
                preferred_element_type=jnp.float32,
            )
            tail = jnp.where(alive, s[width - PIECE :], masked_score)
            scores.append(jnp.concatenate([s[: width - PIECE], tail], axis=0) if count > 1 else tail)
        for h in range(2):
            s = scores[h]
            old = m_s[h]
            new = jnp.maximum(old, jnp.max(s, axis=0, keepdims=True))
            m_s[h] = new
            shrink = jnp.exp2((old - new) * factor)
            p = jnp.exp2((s - new) * factor).astype(jnp.bfloat16)
            v_aug = jnp.concatenate([v_t[h * HD : (h + 1) * HD], ones], axis=0)
            acc_s[h] = acc_s[h] * shrink + jnp.dot(v_aug, p, preferred_element_type=jnp.float32)

    for count in range(1, TOK_DEV // PIECE + 1):
        pl.when(pieces == count)(functools.partial(run, count))

    @pl.when(j == blocks - 1)
    def _():
        both = [acc_s[h][:HD] / acc_s[h][HD : HD + 1] for h in range(2)]
        out_ref[...] = jnp.concatenate(both, axis=0).T.astype(jnp.bfloat16)
        if not finish:
            rows = [m_s[0] * HD ** (-0.5), m_s[1] * HD ** (-0.5)]
            rows += [acc_s[h][HD : HD + 1] for h in range(2)]
            rows += [jnp.zeros((4, out_ref.shape[0]), jnp.float32)]
            stat_ref[...] = jnp.concatenate(rows, axis=0)


def flash(lens, queries, kv, finish, q_first=0):
    rows = queries.shape[0]
    pairs = kv.shape[1] // (2 * PAIR)
    blocks = kv.shape[0] // TOK_DEV
    out_shape = [jax.ShapeDtypeStruct((rows, pairs * PAIR), jnp.bfloat16)]
    out_specs = [pl.BlockSpec((rows, PAIR), lambda p, j, lens: (0, p))]
    if not finish:
        out_shape.append(jax.ShapeDtypeStruct((pairs * 8, rows), jnp.float32))
        out_specs.append(pl.BlockSpec((8, rows), lambda p, j, lens: (p, 0)))
    return pl.pallas_call(
        functools.partial(flash_kernel, blocks=blocks, finish=finish),
        grid_spec=pltpu.PrefetchScalarGridSpec(
            num_scalar_prefetch=1,
            grid=(pairs, blocks),
            in_specs=[
                pl.BlockSpec((rows, PAIR), lambda p, j, lens: (0, q_first + p)),
                pl.BlockSpec((TOK_DEV, PAIR), lambda p, j, lens: (j, p)),
                pl.BlockSpec((TOK_DEV, PAIR), lambda p, j, lens: (j, pairs + p)),
            ],
            out_specs=out_specs,
            scratch_shapes=[
                pltpu.VMEM((2, 1, rows), jnp.float32),
                pltpu.VMEM((2, HD + 16, rows), jnp.float32),
            ],
        ),
        out_shape=out_shape,
        compiler_params=pltpu.CompilerParams(vmem_limit_bytes=32 * 1024 * 1024),
        name="flash",
    )(lens, queries, kv, kv)


def gelu_up(gate, up):
    return (jax.nn.gelu(gate, approximate=True) * up).astype(jnp.bfloat16)


def make_local(seq_size, head_size):
    def from_others(piece):
        got = [piece]
        for shift in range(1, head_size):
            got.append(
                lax.ppermute(piece, "head", [(i, (i + shift) % head_size) for i in range(head_size)])
            )
        return got

    def local(
        tokens,
        norm_attn,
        self_qkv,
        self_out,
        norm_ffn,
        ffn_in,
        ffn_out,
        norm_final,
        pad_lengths,
        targets,
        target_lengths,
        norm_cross,
        cross_query,
        cross_kv,
        cross_out,
    ):
        width = self_qkv.shape[2]
        pairs = width // PAIR
        heads_here = width // HD
        normed = rms_norm(tokens, norm_attn).astype(jnp.bfloat16)
        keys = dot32(normed, self_qkv[1]).astype(jnp.bfloat16)
        values = dot32(normed, self_qkv[2]).astype(jnp.bfloat16)
        gathered = []
        for g in range(pairs):
            cols = slice(g * PAIR, (g + 1) * PAIR)
            piece = jnp.concatenate([keys[:, cols], values[:, cols]], axis=1)
            gathered.append(lax.all_gather(piece, "seq", axis=0, tiled=True))
        queries = dot32(normed, self_qkv[0]).astype(jnp.bfloat16)
        self_outs = from_others(self_out)
        cross_outs = from_others(cross_out)
        attn = None
        for g in range(pairs):
            (context,) = flash(pad_lengths, queries, gathered[g], True, q_first=g)
            rows = slice(g * PAIR, (g + 1) * PAIR)
            sums = [dot32(c, w[rows]) for c, w in zip(from_others(context), self_outs)]
            part = functools.reduce(jnp.add, sums)
            attn = part if attn is None else attn + part
        hidden_in = tokens.astype(jnp.float32) + attn
        ffn_normed = rms_norm(hidden_in, norm_ffn).astype(jnp.bfloat16)
        chunks = 2
        step = tokens.shape[0] // chunks
        encoded_parts = []
        for c in range(chunks):
            some = ffn_normed[c * step : (c + 1) * step]
            activated = gelu_up(dot32(some, ffn_in[0]), dot32(some, ffn_in[1]))
            part = dot32(activated, ffn_out).astype(jnp.bfloat16)
            total = functools.reduce(jnp.add, [x.astype(jnp.float32) for x in from_others(part)])
            final_in = hidden_in[c * step : (c + 1) * step] + total
            encoded_parts.append(rms_norm(final_in, norm_final).astype(jnp.bfloat16))
        encoded = jnp.concatenate(encoded_parts, axis=0)

        target_rows = targets.shape[0]
        cross_normed = rms_norm(targets, norm_cross).astype(jnp.bfloat16)
        cross_queries = dot32(cross_normed, cross_query).astype(jnp.bfloat16)
        cross_keys = dot32(encoded, cross_kv[0]).astype(jnp.bfloat16)
        cross_values = dot32(encoded, cross_kv[1]).astype(jnp.bfloat16)
        place = lax.axis_index("seq")
        own_len = lax.dynamic_slice_in_dim(pad_lengths, place, 1)
        mixed, stats = flash(
            own_len, cross_queries, jnp.concatenate([cross_keys, cross_values], axis=1), False
        )
        stats = stats.reshape(pairs, 4, 2, target_rows)
        top = stats[:, 0].reshape(heads_here, target_rows)
        total = stats[:, 1].reshape(heads_here, target_rows)

        def split(x, count):
            parts = []
            for _ in range(count):
                rounded = lax.reduce_precision(x, 8, 7)
                parts.append(rounded.astype(jnp.bfloat16))
                x = x - rounded
            return parts

        extra = jnp.concatenate(split(top, 3) + split(total, 2), axis=0).T
        pad = -extra.shape[1] % 128
        extra = jnp.pad(extra, ((0, 0), (0, pad)))
        packed = jnp.concatenate([mixed, extra], axis=1)
        own_rows = target_rows // seq_size
        packed = packed.reshape(seq_size, own_rows, packed.shape[1])
        packed = lax.all_to_all(packed, "seq", 0, 0)
        mixed = packed[:, :, :width].astype(jnp.float32)

        def field(i):
            first = width + i * heads_here
            return packed[:, :, first : first + heads_here].astype(jnp.float32)

        top = field(0) + field(1) + field(2)
        total = field(3) + field(4)
        weight = total * jnp.exp(top - jnp.max(top, axis=0, keepdims=True))
        weight = weight / jnp.sum(weight, axis=0, keepdims=True)
        context = jnp.sum(mixed * jnp.repeat(weight, HD, axis=2), axis=0).astype(jnp.bfloat16)
        cross_total = functools.reduce(
            jnp.add, [dot32(c, w) for c, w in zip(from_others(context), cross_outs)]
        )
        slots = place * own_rows + jnp.arange(own_rows, dtype=jnp.int32)
        owner = slots // TGT_LEN
        ids = jnp.arange(target_lengths.shape[0], dtype=jnp.int32)
        limit = jnp.sum(jnp.where(owner[:, None] == ids[None, :], target_lengths[None, :], 0), axis=1)
        target_live = slots % TGT_LEN < limit
        own_targets = lax.dynamic_slice_in_dim(targets, place * own_rows, own_rows, 0)
        decoded = (
            own_targets.astype(jnp.float32) + jnp.where(target_live[:, None], cross_total, 0.0)
        ).astype(jnp.bfloat16)
        return (encoded, lax.all_gather(decoded, "seq", axis=0, tiled=True))

    return local


def solution(mesh):
    placed = (
        P("seq", None),
        P(),
        P(None, None, "head"),
        P("head", None),
        P(),
        P(None, None, "head"),
        P("head", None),
        P(),
        P(),
        P(),
        P(),
        P(),
        P(None, "head"),
        P(None, None, "head"),
        P("head", None),
    )
    return jax.shard_map(
        make_local(mesh.shape["seq"], mesh.shape["head"]),
        mesh=mesh,
        in_specs=placed,
        out_specs=(P("seq", None), P()),
        check_vma=False,
    )
```

```python
import functools
import math

import jax
import jax.numpy as jnp
from jax import lax
from jax.experimental import pallas as pl
from jax.experimental.pallas import tpu as pltpu
from jax.sharding import PartitionSpec as P


HD = 64
TOK_DEV = 512
TGT_LEN = 128
PAIR = 2 * HD
PIECE = 128

epsilon = 1e-06
masked_score = -1e30
LOG2E = math.log2(math.e)


def rms_norm(values, gain_vector):
    widened = values.astype(jnp.float32)
    return (
        widened
        * lax.rsqrt(jnp.mean(widened * widened, axis=-1, keepdims=True) + epsilon)
        * gain_vector
    )


def dot32(a, b):
    return jnp.dot(a, b, preferred_element_type=jnp.float32)


def flash_kernel(lens, q_ref, k_ref, v_ref, *refs, blocks, finish):
    if finish:
        out_ref, m_s, acc_s = refs
    else:
        out_ref, stat_ref, m_s, acc_s = refs
    j = pl.program_id(1)
    factor = HD ** (-0.5) * LOG2E

    @pl.when(j == 0)
    def _():
        m_s[...] = jnp.full(m_s.shape, masked_score, jnp.float32)
        acc_s[...] = jnp.zeros(acc_s.shape, jnp.float32)

    live = lens[j]
    pieces = (live + PIECE - 1) // PIECE

    def run(count):
        width = count * PIECE
        v_t = v_ref[:width, :].T
        ones = jnp.ones((16, width), jnp.bfloat16)
        alive = lax.broadcasted_iota(jnp.int32, (PIECE, 1), 0) < live - (width - PIECE)
        scores = []
        for h in range(2):
            cols = slice(h * HD, (h + 1) * HD)
            s = lax.dot_general(
                k_ref[:width, cols],
                q_ref[:, cols],
                (((1,), (1,)), ((), ())),
                preferred_element_type=jnp.float32,
            )
            tail = jnp.where(alive, s[width - PIECE :], masked_score)
            scores.append(jnp.concatenate([s[: width - PIECE], tail], axis=0) if count > 1 else tail)
        for h in range(2):
            s = scores[h]
            old = m_s[h]
            new = jnp.maximum(old, jnp.max(s, axis=0, keepdims=True))
            m_s[h] = new
            shrink = jnp.exp2((old - new) * factor)
            p = jnp.exp2((s - new) * factor).astype(jnp.bfloat16)
            v_aug = jnp.concatenate([v_t[h * HD : (h + 1) * HD], ones], axis=0)
            acc_s[h] = acc_s[h] * shrink + jnp.dot(v_aug, p, preferred_element_type=jnp.float32)

    for count in range(1, TOK_DEV // PIECE + 1):
        pl.when(pieces == count)(functools.partial(run, count))

    @pl.when(j == blocks - 1)
    def _():
        both = [acc_s[h][:HD] / acc_s[h][HD : HD + 1] for h in range(2)]
        out_ref[...] = jnp.concatenate(both, axis=0).T.astype(jnp.bfloat16)
        if not finish:
            rows = [m_s[0] * HD ** (-0.5), m_s[1] * HD ** (-0.5)]
            rows += [acc_s[h][HD : HD + 1] for h in range(2)]
            rows += [jnp.zeros((4, out_ref.shape[0]), jnp.float32)]
            stat_ref[...] = jnp.concatenate(rows, axis=0)


def flash(lens, queries, kv, finish, q_first=0):
    rows = queries.shape[0]
    pairs = kv.shape[1] // (2 * PAIR)
    blocks = kv.shape[0] // TOK_DEV
    out_shape = [jax.ShapeDtypeStruct((rows, pairs * PAIR), jnp.bfloat16)]
    out_specs = [pl.BlockSpec((rows, PAIR), lambda p, j, lens: (0, p))]
    if not finish:
        out_shape.append(jax.ShapeDtypeStruct((pairs * 8, rows), jnp.float32))
        out_specs.append(pl.BlockSpec((8, rows), lambda p, j, lens: (p, 0)))
    return pl.pallas_call(
        functools.partial(flash_kernel, blocks=blocks, finish=finish),
        grid_spec=pltpu.PrefetchScalarGridSpec(
            num_scalar_prefetch=1,
            grid=(pairs, blocks),
            in_specs=[
                pl.BlockSpec((rows, PAIR), lambda p, j, lens: (0, q_first + p)),
                pl.BlockSpec((TOK_DEV, PAIR), lambda p, j, lens: (j, p)),
                pl.BlockSpec((TOK_DEV, PAIR), lambda p, j, lens: (j, pairs + p)),
            ],
            out_specs=out_specs,
            scratch_shapes=[
                pltpu.VMEM((2, 1, rows), jnp.float32),
                pltpu.VMEM((2, HD + 16, rows), jnp.float32),
            ],
        ),
        out_shape=out_shape,
        compiler_params=pltpu.CompilerParams(vmem_limit_bytes=32 * 1024 * 1024),
        name="flash",
    )(lens, queries, kv, kv)


def gelu_up(gate, up):
    return (jax.nn.gelu(gate, approximate=True) * up).astype(jnp.bfloat16)


def make_local(seq_size, head_size):
    def from_others(piece):
        got = [piece]
        for shift in range(1, head_size):
            got.append(
                lax.ppermute(piece, "head", [(i, (i + shift) % head_size) for i in range(head_size)])
            )
        return got

    def local(
        tokens,
        norm_attn,
        self_qkv,
        self_out,
        norm_ffn,
        ffn_in,
        ffn_out,
        norm_final,
        pad_lengths,
        targets,
        target_lengths,
        norm_cross,
        cross_query,
        cross_kv,
        cross_out,
    ):
        width = self_qkv.shape[2]
        pairs = width // PAIR
        heads_here = width // HD
        normed = rms_norm(tokens, norm_attn).astype(jnp.bfloat16)
        keys = dot32(normed, self_qkv[1]).astype(jnp.bfloat16)
        values = dot32(normed, self_qkv[2]).astype(jnp.bfloat16)
        gathered = []
        groups = [(0, pairs - 1), (pairs - 1, pairs)] if pairs > 1 else [(0, pairs)]
        for first, last in groups:
            cols = slice(first * PAIR, last * PAIR)
            piece = jnp.concatenate([keys[:, cols], values[:, cols]], axis=1)
            gathered.append(lax.all_gather(piece, "seq", axis=0, tiled=True))
        queries = dot32(normed, self_qkv[0]).astype(jnp.bfloat16)
        self_outs = from_others(self_out)
        cross_outs = from_others(cross_out)
        attn = None
        for (first, last), kv in zip(groups, gathered):
            (context,) = flash(pad_lengths, queries, kv, True, q_first=first)
            rows = slice(first * PAIR, last * PAIR)
            sums = [dot32(c, w[rows]) for c, w in zip(from_others(context), self_outs)]
            part = functools.reduce(jnp.add, sums)
            attn = part if attn is None else attn + part
        hidden_in = tokens.astype(jnp.float32) + attn
        ffn_normed = rms_norm(hidden_in, norm_ffn).astype(jnp.bfloat16)
        chunks = 2
        step = tokens.shape[0] // chunks
        encoded_parts = []
        for c in range(chunks):
            some = ffn_normed[c * step : (c + 1) * step]
            activated = gelu_up(dot32(some, ffn_in[0]), dot32(some, ffn_in[1]))
            part = dot32(activated, ffn_out).astype(jnp.bfloat16)
            total = functools.reduce(jnp.add, [x.astype(jnp.float32) for x in from_others(part)])
            final_in = hidden_in[c * step : (c + 1) * step] + total
            encoded_parts.append(rms_norm(final_in, norm_final).astype(jnp.bfloat16))
        encoded = jnp.concatenate(encoded_parts, axis=0)

        target_rows = targets.shape[0]
        cross_normed = rms_norm(targets, norm_cross).astype(jnp.bfloat16)
        cross_queries = dot32(cross_normed, cross_query).astype(jnp.bfloat16)
        cross_keys = dot32(encoded, cross_kv[0]).astype(jnp.bfloat16)
        cross_values = dot32(encoded, cross_kv[1]).astype(jnp.bfloat16)
        place = lax.axis_index("seq")
        own_len = lax.dynamic_slice_in_dim(pad_lengths, place, 1)
        mixed, stats = flash(
            own_len, cross_queries, jnp.concatenate([cross_keys, cross_values], axis=1), False
        )
        stats = stats.reshape(pairs, 4, 2, target_rows)
        top = stats[:, 0].reshape(heads_here, target_rows)
        total = stats[:, 1].reshape(heads_here, target_rows)

        def split(x, count):
            parts = []
            for _ in range(count):
                rounded = lax.reduce_precision(x, 8, 7)
                parts.append(rounded.astype(jnp.bfloat16))
                x = x - rounded
            return parts

        extra = jnp.concatenate(split(top, 3) + split(total, 2), axis=0).T
        pad = -extra.shape[1] % 128
        extra = jnp.pad(extra, ((0, 0), (0, pad)))
        packed = jnp.concatenate([mixed, extra], axis=1)
        own_rows = target_rows // seq_size
        packed = packed.reshape(seq_size, own_rows, packed.shape[1])
        packed = lax.all_to_all(packed, "seq", 0, 0)
        mixed = packed[:, :, :width].astype(jnp.float32)

        def field(i):
            first = width + i * heads_here
            return packed[:, :, first : first + heads_here].astype(jnp.float32)

        top = field(0) + field(1) + field(2)
        total = field(3) + field(4)
        weight = total * jnp.exp(top - jnp.max(top, axis=0, keepdims=True))
        weight = weight / jnp.sum(weight, axis=0, keepdims=True)
        context = jnp.sum(mixed * jnp.repeat(weight, HD, axis=2), axis=0).astype(jnp.bfloat16)
        cross_total = functools.reduce(
            jnp.add, [dot32(c, w) for c, w in zip(from_others(context), cross_outs)]
        )
        slots = place * own_rows + jnp.arange(own_rows, dtype=jnp.int32)
        owner = slots // TGT_LEN
        ids = jnp.arange(target_lengths.shape[0], dtype=jnp.int32)
        limit = jnp.sum(jnp.where(owner[:, None] == ids[None, :], target_lengths[None, :], 0), axis=1)
        target_live = slots % TGT_LEN < limit
        own_targets = lax.dynamic_slice_in_dim(targets, place * own_rows, own_rows, 0)
        decoded = (
            own_targets.astype(jnp.float32) + jnp.where(target_live[:, None], cross_total, 0.0)
        ).astype(jnp.bfloat16)
        copies = jnp.broadcast_to(decoded[None], (seq_size,) + decoded.shape)
        decoded = lax.all_to_all(copies, "seq", 0, 0).reshape(targets.shape)
        return (encoded, decoded)

    return local


def solution(mesh):
    placed = (
        P("seq", None),
        P(),
        P(None, None, "head"),
        P("head", None),
        P(),
        P(None, None, "head"),
        P("head", None),
        P(),
        P(),
        P(),
        P(),
        P(),
        P(None, "head"),
        P(None, None, "head"),
        P("head", None),
    )
    return jax.shard_map(
        make_local(mesh.shape["seq"], mesh.shape["head"]),
        mesh=mesh,
        in_specs=placed,
        out_specs=(P("seq", None), P()),
        check_vma=False,
    )
```
